32 devices in a mesh: fsdp: 4 (over z), tp: 8 (over y, x, core).
Axes of the slice: x: 2, y: 2, z: 4, core: 2. Of those that a mesh axis runs over, the one named last changes fastest.
Arguments:
- tokens: bfloat16 [3008, 4096], P('fsdp', 'tp'), may hold values from -6 to 6
- norm_gain: float32 [4096], replicated, may hold values from 0.5 to 1.5
- base_gate: bfloat16 [4096, 12288], P(None, 'tp'), may hold values from -0.09375 to 0.09375
- base_up: bfloat16 [4096, 12288], P(None, 'tp'), may hold values from -0.09375 to 0.09375
- base_down: bfloat16 [12288, 4096], P('tp'), may hold values from -0.0546875 to 0.0546875
- code_gate: bfloat16 [4096, 12288], P(('fsdp', 'tp')), may hold values from -4 to 4
- code_up: bfloat16 [4096, 12288], P(('fsdp', 'tp')), may hold values from -4 to 4
- scale_gate: float32 [4096, 96], P(('fsdp', 'tp')), may hold values from 0.005 to 0.05
- scale_up: float32 [4096, 96], P(('fsdp', 'tp')), may hold values from 0.005 to 0.05
- code_down: bfloat16 [12288, 4096], P(None, ('fsdp', 'tp')), may hold values from -4 to 4
- scale_down: float32 [96, 4096], P(None, ('fsdp', 'tp')), may hold values from 0.005 to 0.05
- cu_seqlens: int32 [4, 9], P('fsdp'), may hold values from 0 to 752, as said below
Outputs:
- mixed: bfloat16 [3008, 4096], P('fsdp', 'tp')
- seq_means: float32 [32, 4096], P('fsdp', 'tp')
The draws below stay inside these ranges and needn't reach their ends.
Inputs may be any that keep to these rules, and one draw needn't show every extreme that they name: `cu_seqlens`: each row starts at 0 and rises strictly; its last entry is the group's live tokens, which fill the first slots of its 752. Over all groups the live tokens add up to exactly 1536, and some group has exactly 752.
All inputs are finite; a program needn't handle non-finite values.
Results may differ from the reference program's by a relative error of at most 0.023.
Values may be sent and summed in bfloat16 or wider, within the bound.
A program may use at most 256 MiB of HBM per device.

```python
import math
import jax
import jax.numpy as jnp
from jax import lax

D = 4096
FF = 12288
BLK = 128
SEQS = 8
BAL = 384
CAP = 752
GROUPS = 4
TOKENS = 3008
N_TP = 8


def draw_cu_seqlens(key, part):
    key_pairs = jax.random.fold_in(key, 11)
    key_order = jax.random.fold_in(key, 12)
    key_cuts = jax.random.fold_in(key, 13)
    spread = jax.random.randint(key_pairs, (GROUPS // 2,), 0, BAL - 2 * SEQS + 1).astype(jnp.int32)
    spread = spread.at[0].set(BAL - 2 * SEQS)
    counts = jnp.stack([BAL + spread, BAL - spread], axis=1).reshape(GROUPS)
    counts = counts[jax.random.permutation(key_order, GROUPS)]
    upper_bound = (counts - SEQS + 1)[:, None]
    cut_points = jax.random.randint(key_cuts, (GROUPS, SEQS - 1), 0, upper_bound).astype(jnp.int32)
    cut_points = jnp.sort(cut_points, axis=1) + jnp.arange(1, SEQS, dtype=jnp.int32)[None, :]
    leading = jnp.zeros((GROUPS, 1), jnp.int32)
    return jnp.concatenate([leading, cut_points, counts[:, None].astype(jnp.int32)], axis=1)


def levels(key, dims, cuts, low, high):
    def one(axis_at, shards_of):
        steps = jax.random.uniform(jax.random.fold_in(jax.random.fold_in(key, 6), axis_at), (shards_of,), jnp.float32, low / len(cuts), high / len(cuts))
        return jnp.repeat(jnp.exp(steps), dims[axis_at] // shards_of).reshape((-1,) + (1,) * (len(dims) - axis_at - 1))

    factor_of = one(*cuts[0])
    for cut in cuts[1:]:
        factor_of = factor_of * one(*cut)
    return factor_of


def gaussian(key, dims, width, reach, shards=(), kind=jnp.bfloat16):
    values = jax.random.normal(key, dims, jnp.float32) * width
    if len(shards) > 0:
        values = levels(key, dims, shards, -0.22, 0.18) * values
    return jnp.clip(values, min=-reach, max=reach).astype(kind)


def setup_inputs(seed: int = 0) -> dict:
    seeds = jax.random.split(jax.random.key(seed), 13)
    tokens = gaussian(seeds[0], (TOKENS, D), 1.0, 6.0, ((0, 4), (1, 8)))
    norm_gain = jnp.clip(jax.random.uniform(seeds[1], (D,), jnp.float32, 0.5, 1.5), 0.5, 1.5)
    base_gate = gaussian(seeds[2], (D, FF), D ** -0.5, 0.09375, ((1, 8),))
    base_up = gaussian(seeds[3], (D, FF), D ** -0.5, 0.09375, ((1, 8),))
    base_down = gaussian(seeds[4], (FF, D), FF ** -0.5, 0.0546875, ((0, 8),))
    code_gate = gaussian(seeds[5], (D, FF), 1.0, 4.0, ((0, 32),))
    code_up = gaussian(seeds[6], (D, FF), 1.0, 4.0, ((0, 32),))
    scale_gate = jnp.clip(jnp.exp(math.log(0.05) - 2.3025851 * jax.random.uniform(seeds[7], (D, FF // BLK), jnp.float32) ** levels(seeds[7], (D, FF // BLK), ((0, 32),), -0.2, 0.2)), 0.005, 0.05)
    scale_up = jnp.clip(jnp.exp(math.log(0.05) - 2.3025851 * jax.random.uniform(seeds[8], (D, FF // BLK), jnp.float32) ** levels(seeds[8], (D, FF // BLK), ((0, 32),), -0.2, 0.2)), 0.005, 0.05)
    code_down = gaussian(seeds[9], (FF, D), 1.0, 4.0, ((1, 32),))
    scale_down = jnp.clip(jnp.exp(math.log(0.05) - 2.3025851 * jax.random.uniform(seeds[10], (FF // BLK, D), jnp.float32) ** levels(seeds[10], (FF // BLK, D), ((1, 32),), -0.2, 0.2)), 0.005, 0.05)
    cu_seqlens = draw_cu_seqlens(jax.random.fold_in(seeds[12], 71), 0)
    return {"tokens": tokens, "norm_gain": norm_gain, "base_gate": base_gate, "base_up": base_up, "base_down": base_down, "code_gate": code_gate, "code_up": code_up, "scale_gate": scale_gate, "scale_up": scale_up, "code_down": code_down, "scale_down": scale_down, "cu_seqlens": cu_seqlens}


EPSILON = 1e-06

def reference(tokens, norm_gain, base_gate, base_up, base_down, code_gate, code_up, scale_gate, scale_up, code_down, scale_down, cu_seqlens):
    w_gate = (base_gate.astype(jnp.float32) + code_gate.astype(jnp.float32) * jnp.repeat(scale_gate, BLK, axis=1)).astype(jnp.bfloat16)
    w_up = (base_up.astype(jnp.float32) + code_up.astype(jnp.float32) * jnp.repeat(scale_up, BLK, axis=1)).astype(jnp.bfloat16)
    w_down = (base_down.astype(jnp.float32) + code_down.astype(jnp.float32) * jnp.repeat(scale_down, BLK, axis=0)).astype(jnp.bfloat16)
    slice_width = FF // N_TP
    down_slices = w_down.reshape(N_TP, slice_width, D)
    stacked = tokens.reshape(GROUPS, CAP, D)
    positions = jnp.arange(CAP, dtype=jnp.int32)

    def one_group(operands):
        rows_in, bounds = operands
        widened = rows_in.astype(jnp.float32)
        inverse = lax.rsqrt(lax.optimization_barrier(jnp.mean(widened * widened, axis=1, keepdims=True)) + EPSILON)
        normed = (widened * inverse * norm_gain[None, :]).astype(jnp.bfloat16)
        gate_out = jnp.dot(normed, w_gate, preferred_element_type=jnp.float32)
        up_out = jnp.dot(normed, w_up, preferred_element_type=jnp.float32)
        hidden = (jax.nn.silu(gate_out) * up_out).astype(jnp.bfloat16)
        hidden_slices = hidden.reshape(CAP, N_TP, slice_width).transpose(1, 0, 2)

        def add_slice(running, pair):
            partial_value = jnp.dot(pair[0], pair[1], preferred_element_type=jnp.float32).astype(jnp.bfloat16)
            return (running + partial_value.astype(jnp.float32), None)
        summed, _ = lax.scan(add_slice, jnp.zeros((CAP, D), jnp.float32), (hidden_slices, down_slices))
        mixed_rows = (widened + summed).astype(jnp.bfloat16)
        live_count = bounds[SEQS]
        mixed_rows = jnp.where((positions < live_count)[:, None], mixed_rows, jnp.zeros((), jnp.bfloat16))
        member = (positions[None, :] >= bounds[:-1, None]) & (positions[None, :] < bounds[1:, None])
        seq_sums = jnp.dot(member.astype(jnp.bfloat16), mixed_rows, preferred_element_type=jnp.float32)
        lengths = (bounds[1:] - bounds[:-1]).astype(jnp.float32)
        return (mixed_rows, seq_sums / lengths[:, None])
    mixed_all, means_all = lax.map(one_group, (stacked, cu_seqlens))
    return (mixed_all.reshape(GROUPS * CAP, D), means_all.reshape(GROUPS * SEQS, D))
```

```python
import jax
import jax.numpy as jnp
from jax import lax
from jax.sharding import PartitionSpec as P

SEQS = 8
EPSILON = 1e-06
F32, BF16 = jnp.float32, jnp.bfloat16


def dequant_rows(base_part, code_part, scales):
    rows, cols = code_part.shape
    blocks = scales.shape[1]
    delta = code_part.astype(F32).reshape(rows, blocks, cols // blocks) * scales[:, :, None]
    return (base_part.astype(F32) + delta.reshape(rows, cols)).astype(BF16)


def dequant_cols(base_part, code_part, scales):
    rows, cols = code_part.shape
    blocks = scales.shape[0]
    delta = code_part.astype(F32).reshape(blocks, rows // blocks, cols) * scales[:, None, :]
    return (base_part.astype(F32) + delta.reshape(rows, cols)).astype(BF16)


def swap_up(part, axis_name="tp"):
    return lax.all_to_all(part, axis_name, split_axis=1, concat_axis=0, tiled=True)


def swap_down(part):
    return lax.all_to_all(part, "tp", split_axis=0, concat_axis=1, tiled=True)


def shards(tokens, norm_gain, base_gate, base_up, base_down, code_gate, code_up,
           scale_gate, scale_up, code_down, scale_down, cu_seqlens):
    groups = lax.axis_size("fsdp")
    slices = lax.axis_size("tp")
    me_f = lax.axis_index("fsdp")
    me_t = lax.axis_index("tp")
    cap, feat = tokens.shape
    width = base_gate.shape[0]
    depth = width // groups
    units = base_gate.shape[1]
    live_all = groups * (cap // 2 + SEQS)
    grain = 16 * slices
    capp = -(-cap // grain) * grain
    part = capp // slices

    padded = jnp.pad(tokens, ((0, capp - cap), (0, 0)))
    rows_full = lax.all_to_all(padded, "tp", split_axis=0, concat_axis=1, tiled=True)
    wide = rows_full.astype(F32)
    inverse = lax.rsqrt(jnp.mean(wide * wide, axis=1, keepdims=True) + EPSILON)
    normed = (wide * inverse * norm_gain[None, :]).astype(BF16)
    block = swap_up(normed, "fsdp")
    every = lax.all_gather(block, "tp", axis=0, tiled=True)

    bounds_all = lax.all_gather(cu_seqlens, "fsdp", axis=0, tiled=True)
    counts = bounds_all[:, SEQS]
    ends = jnp.cumsum(counts)
    starts = ends - counts
    place = jnp.arange(live_all, dtype=jnp.int32)
    group_of = jnp.sum((place[:, None] >= ends[None, :]).astype(jnp.int32), axis=1)
    group_of = jnp.minimum(group_of, groups - 1)
    slot = place - jnp.take(starts, group_of)
    source = (slot // part) * (groups * part) + group_of * part + slot % part
    pick = (source[:, None] == jnp.arange(slices * groups * part, dtype=jnp.int32)[None, :]).astype(BF16)
    packed = jnp.dot(pick, every, preferred_element_type=F32).astype(BF16)

    gate_rows = lax.dynamic_slice_in_dim(base_gate, me_f * depth, depth, 0)
    up_rows = lax.dynamic_slice_in_dim(base_up, me_f * depth, depth, 0)
    w_gate = dequant_rows(gate_rows, swap_up(code_gate), swap_up(scale_gate))
    w_up = dequant_rows(up_rows, swap_up(code_up), swap_up(scale_up))
    partial = jnp.concatenate(
        [jnp.dot(packed, w_gate, preferred_element_type=F32).astype(BF16),
         jnp.dot(packed, w_up, preferred_element_type=F32).astype(BF16)], axis=1)
    summed = lax.psum_scatter(partial, "fsdp", scatter_dimension=0, tiled=True).astype(F32)
    hidden = (jax.nn.silu(summed[:, :units]) * summed[:, units:]).astype(BF16)
    hidden_all = lax.all_gather(hidden, "fsdp", axis=0, tiled=True)

    down_cols = lax.dynamic_slice_in_dim(base_down, me_f * depth, depth, 1)
    w_down = dequant_cols(down_cols, swap_down(code_down), swap_down(scale_down))
    out_part = jnp.dot(hidden_all, w_down, preferred_element_type=F32).astype(BF16)
    out_cols = lax.psum_scatter(out_part, "tp", scatter_dimension=1, tiled=True)
    narrow = out_cols.shape[1]

    grp = jnp.arange(groups, dtype=jnp.int32)
    slots = jnp.arange(cap, dtype=jnp.int32)
    wanted = jnp.where(slots[None, :] < counts[:, None], starts[:, None] + slots[None, :], -1)
    spread = (wanted.reshape(-1)[:, None] == place[None, :]).astype(BF16)
    placed_rows = jnp.dot(spread, out_cols, preferred_element_type=F32).astype(BF16)
    mine = lax.all_to_all(placed_rows.reshape(groups, cap, narrow), "fsdp", split_axis=0, concat_axis=0, tiled=True)
    ratio = slices // groups
    span = slices // ratio
    half = me_t // span
    pick_half = (jnp.arange(ratio) == half)[None, :, None, None]
    outgoing = jnp.where(pick_half, mine[:, None], jnp.zeros((), BF16)).reshape(slices, cap, narrow)
    incoming = lax.all_to_all(outgoing, "tp", split_axis=0, concat_axis=0, tiled=True)
    take_from = lax.dynamic_slice_in_dim(incoming, (me_t % ratio) * span, span, 0)
    summed_out = take_from.transpose(1, 0, 2).reshape(cap, feat).astype(F32)

    bounds = cu_seqlens[0]
    live_count = bounds[SEQS]
    mixed = (tokens.astype(F32) + summed_out).astype(BF16)
    mixed = jnp.where((slots < live_count)[:, None], mixed, jnp.zeros((), BF16))
    member = (slots[None, :] >= bounds[:-1, None]) & (slots[None, :] < bounds[1:, None])
    seq_sums = jnp.dot(member.astype(BF16), mixed, preferred_element_type=F32)
    lengths = (bounds[1:] - bounds[:-1]).astype(F32)
    return mixed, seq_sums / lengths[:, None]


def solution(mesh):
    placed = (
        P("fsdp", "tp"), P(), P(None, "tp"), P(None, "tp"), P("tp", None),
        P(("fsdp", "tp"), None), P(("fsdp", "tp"), None),
        P(("fsdp", "tp"), None), P(("fsdp", "tp"), None),
        P(None, ("fsdp", "tp")), P(None, ("fsdp", "tp")), P("fsdp", None),
    )
    return jax.shard_map(shards, mesh=mesh, in_specs=placed,
                         out_specs=(P("fsdp", "tp"), P("fsdp", "tp")), check_vma=False)
```

```python
import jax
import jax.numpy as jnp
from jax import lax
from jax.sharding import PartitionSpec as P

SEQS = 8
EPSILON = 1e-06
F32, BF16 = jnp.float32, jnp.bfloat16


def dequant_rows(base_part, code_part, scales):
    rows, cols = code_part.shape
    blocks = scales.shape[1]
    delta = code_part.astype(F32).reshape(rows, blocks, cols // blocks) * scales[:, :, None]
    return (base_part.astype(F32) + delta.reshape(rows, cols)).astype(BF16)


def dequant_cols(base_part, code_part, scales):
    rows, cols = code_part.shape
    blocks = scales.shape[0]
    delta = code_part.astype(F32).reshape(blocks, rows // blocks, cols) * scales[:, None, :]
    return (base_part.astype(F32) + delta.reshape(rows, cols)).astype(BF16)


def swap_up(part, axis_name="tp"):
    return lax.all_to_all(part, axis_name, split_axis=1, concat_axis=0, tiled=True)


def swap_down(part):
    return lax.all_to_all(part, "tp", split_axis=0, concat_axis=1, tiled=True)


def shards(tokens, norm_gain, base_gate, base_up, base_down, code_gate, code_up,
           scale_gate, scale_up, code_down, scale_down, cu_seqlens):
    groups = lax.axis_size("fsdp")
    slices = lax.axis_size("tp")
    me_f = lax.axis_index("fsdp")
    me_t = lax.axis_index("tp")
    cap, feat = tokens.shape
    width = base_gate.shape[0]
    depth = width // groups
    units = base_gate.shape[1]
    live_all = groups * (cap // 2 + SEQS)
    grain = 16 * slices
    capp = -(-cap // grain) * grain
    part = capp // slices

    padded = jnp.pad(tokens, ((0, capp - cap), (0, 0)))
    rows_full = lax.all_to_all(padded, "tp", split_axis=0, concat_axis=1, tiled=True)
    wide = rows_full.astype(F32)
    inverse = lax.rsqrt(jnp.mean(wide * wide, axis=1, keepdims=True) + EPSILON)
    normed = (wide * inverse * norm_gain[None, :]).astype(BF16)
    block = swap_up(normed, "fsdp")
    every = lax.all_gather(block, "tp", axis=0, tiled=True)

    bounds_all = lax.all_gather(cu_seqlens, "fsdp", axis=0, tiled=True)
    counts = bounds_all[:, SEQS]
    ends = jnp.cumsum(counts)
    starts = ends - counts
    place = jnp.arange(live_all, dtype=jnp.int32)
    group_of = jnp.sum((place[:, None] >= ends[None, :]).astype(jnp.int32), axis=1)
    group_of = jnp.minimum(group_of, groups - 1)
    slot = place - jnp.take(starts, group_of)
    source = (slot // part) * (groups * part) + group_of * part + slot % part
    pick = (source[:, None] == jnp.arange(slices * groups * part, dtype=jnp.int32)[None, :]).astype(BF16)
    packed = jnp.dot(pick, every, preferred_element_type=F32).astype(BF16)

    gate_rows = lax.dynamic_slice_in_dim(base_gate, me_f * depth, depth, 0)
    up_rows = lax.dynamic_slice_in_dim(base_up, me_f * depth, depth, 0)
    w_gate = dequant_rows(gate_rows, swap_up(code_gate), swap_up(scale_gate))
    w_up = dequant_rows(up_rows, swap_up(code_up), swap_up(scale_up))
    gate_part = jnp.dot(packed, w_gate, preferred_element_type=F32).astype(BF16)
    up_part = jnp.dot(packed, w_up, preferred_element_type=F32).astype(BF16)
    up_part, code_down = lax.optimization_barrier((up_part, code_down))
    gate_sum = lax.psum_scatter(gate_part, "fsdp", scatter_dimension=0, tiled=True)
    up_sum = lax.psum_scatter(up_part, "fsdp", scatter_dimension=0, tiled=True)
    down_codes, down_scales = swap_down(code_down), swap_down(scale_down)
    gate_sum, up_sum, down_codes, down_scales = lax.optimization_barrier(
        (gate_sum, up_sum, down_codes, down_scales))
    hidden = (jax.nn.silu(gate_sum.astype(F32)) * up_sum.astype(F32)).astype(BF16)
    hidden_all = lax.all_gather(hidden, "fsdp", axis=0, tiled=True)

    down_cols = lax.dynamic_slice_in_dim(base_down, me_f * depth, depth, 1)
    w_down = dequant_cols(down_cols, down_codes, down_scales)
    out_part = jnp.dot(hidden_all, w_down, preferred_element_type=F32).astype(BF16)
    out_cols = lax.psum_scatter(out_part, "tp", scatter_dimension=1, tiled=True)
    narrow = out_cols.shape[1]

    grp = jnp.arange(groups, dtype=jnp.int32)
    slots = jnp.arange(cap, dtype=jnp.int32)
    wanted = jnp.where(slots[None, :] < counts[:, None], starts[:, None] + slots[None, :], -1)
    spread = (wanted.reshape(-1)[:, None] == place[None, :]).astype(BF16)
    placed_rows = jnp.dot(spread, out_cols, preferred_element_type=F32).astype(BF16)
    mine = lax.all_to_all(placed_rows.reshape(groups, cap, narrow), "fsdp", split_axis=0, concat_axis=0, tiled=True)
    ratio = slices // groups
    span = slices // ratio
    half = me_t // span
    pick_half = (jnp.arange(ratio) == half)[None, :, None, None]
    outgoing = jnp.where(pick_half, mine[:, None], jnp.zeros((), BF16)).reshape(slices, cap, narrow)
    incoming = lax.all_to_all(outgoing, "tp", split_axis=0, concat_axis=0, tiled=True)
    take_from = lax.dynamic_slice_in_dim(incoming, (me_t % ratio) * span, span, 0)
    summed_out = take_from.transpose(1, 0, 2).reshape(cap, feat).astype(F32)

    bounds = cu_seqlens[0]
    live_count = bounds[SEQS]
    mixed = (tokens.astype(F32) + summed_out).astype(BF16)
    mixed = jnp.where((slots < live_count)[:, None], mixed, jnp.zeros((), BF16))
    member = (slots[None, :] >= bounds[:-1, None]) & (slots[None, :] < bounds[1:, None])
    seq_sums = jnp.dot(member.astype(BF16), mixed, preferred_element_type=F32)
    lengths = (bounds[1:] - bounds[:-1]).astype(F32)
    return mixed, seq_sums / lengths[:, None]


def solution(mesh):
    placed = (
        P("fsdp", "tp"), P(), P(None, "tp"), P(None, "tp"), P("tp", None),
        P(("fsdp", "tp"), None), P(("fsdp", "tp"), None),
        P(("fsdp", "tp"), None), P(("fsdp", "tp"), None),
        P(None, ("fsdp", "tp")), P(None, ("fsdp", "tp")), P("fsdp", None),
    )
    return jax.shard_map(shards, mesh=mesh, in_specs=placed,
                         out_specs=(P("fsdp", "tp"), P("fsdp", "tp")), check_vma=False)
```
